32 devices in a mesh: batch: 16 (over z, y, core), seq: 2 (over x).
Axes of the slice: x: 2, y: 2, z: 4, core: 2. Of those that a mesh axis runs over, the one named last changes fastest.
Arguments:
- queries: bfloat16 [4096, 4096], P(('batch', 'seq')), parts along dimension 0, may hold values from -130 to 130
- span_keys: bfloat16 [4096, 1024], P(('batch', 'seq')), parts along dimension 0, may hold values from -6 to 6
- span_values: bfloat16 [4096, 1024], P(('batch', 'seq')), parts along dimension 0, may hold values from -6 to 6
- cache_keys: bfloat16 [65536, 1024], P(('batch', 'seq')), parts along dimension 0, may hold values from -6 to 6
- cache_values: bfloat16 [65536, 1024], P(('batch', 'seq')), parts along dimension 0, may hold values from -6 to 6
- span_start: int32 [16], P('batch'), parts along dimension 0, may hold values from 2048 to 16383, as said below
- prompt_length: int32 [16], P('batch'), parts along dimension 0, may hold values from 2112 to 16639, as said below
- window_size: int32 [16], P('batch'), parts along dimension 0, may hold values from 2048 to 4096
Outputs:
- attended: bfloat16 [4096, 4096], P(('batch', 'seq')), parts along dimension 0
The draws below stay inside these ranges and needn't reach their ends.
There are 16 independent parts, one for each index of `batch`. The reference program is written for one: setup_inputs(seed, part) draws one part's arguments, and reference() takes and returns one part's arrays. A program takes and returns all parts, laid end to end along the dimension named above; each array names one. Nothing has to cross between parts.
Inputs may be any that keep to these rules, and one draw needn't show every extreme that they name: Cache row j holds position span_start - 4096 + j and is unused where that is negative. `prompt_length`: lies between span_start + 64 and span_start + 256; block rows at or past it are padding.
All inputs are finite; a program needn't handle non-finite values.
Results may differ from the reference program's by a relative error of at most 0.0065.
Values may be sent and summed in bfloat16 or wider, within the bound.
A program may use at most 128 MiB of HBM per device.

```python
import jax
import jax.numpy as jnp
from jax import lax

H = 32
KVH = 8
HD = 128
WINDOW = 4096
SPAN = 256


def start_and_length(key):
    first, second = jax.random.split(jax.random.fold_in(key, 11))
    begin = jax.random.randint(first, (1,), WINDOW // 2, 4 * WINDOW, dtype=jnp.int32)
    count = jax.random.randint(second, (1,), SPAN // 4, SPAN + 1, dtype=jnp.int32)
    return (begin, begin + count)


def draw_span_start(key, part):
    return start_and_length(key)[0]


def draw_prompt_length(key, part):
    return start_and_length(key)[1]


def draw_window_size(key, part):
    return jax.random.randint(jax.random.fold_in(key, 41), (1,), WINDOW // 2, WINDOW + 1, dtype=jnp.int32)


def draw_span_keys(key, part):
    base = jax.random.truncated_normal(jax.random.fold_in(key, 21), -5.0, 5.0, (SPAN, KVH * HD), jnp.float32)
    return base.astype(jnp.bfloat16)


def draw_queries(key, part):
    return jax.random.truncated_normal(jax.random.fold_in(key, 31), -5.0, 5.0, (SPAN, H * HD), jnp.float32).astype(jnp.bfloat16)


def block_scale(stream_key, dims, pieces, low, high):
    loudness, own = 1.0, jax.random.fold_in(stream_key, 6)
    for position, shards_of in pieces:
        draws = jnp.exp(jax.random.uniform(jax.random.fold_in(own, position), (shards_of,), jnp.float32, low / len(pieces), high / len(pieces)))
        loudness = loudness * jnp.repeat(draws, dims[position] // shards_of).reshape([-1 if axis == position else 1 for axis in range(len(dims))])
    return loudness


def bell_draw(stream_key, dims, spread, reach, cuts=(), kind=jnp.bfloat16):
    factor_of = block_scale(stream_key, dims, cuts, -0.22, 0.18) if cuts else 1.0
    array = jax.random.normal(stream_key, dims, jnp.float32) * spread * factor_of
    return jnp.minimum(jnp.maximum(array, -reach), reach).astype(kind)


def setup_inputs(seed: int = 0, part: int = 0) -> dict:
    seeds = jax.random.split(jax.random.key(seed), 9)
    part_keys = jax.random.split(jax.random.fold_in(seeds[8], part), 9)
    return {
        "queries": draw_queries(jax.random.fold_in(jax.random.fold_in(seeds[8], part), 71), part),
        "span_keys": draw_span_keys(jax.random.fold_in(jax.random.fold_in(seeds[8], part), 71), part),
        "span_values": bell_draw(part_keys[2], (SPAN, KVH * HD), 1.0, 6.0, ((0, 2),)),
        "cache_keys": bell_draw(part_keys[3], (WINDOW, KVH * HD), 1.0, 6.0, ((0, 2),)),
        "cache_values": bell_draw(part_keys[4], (WINDOW, KVH * HD), 1.0, 6.0, ((0, 2),)),
        "span_start": draw_span_start(jax.random.fold_in(jax.random.fold_in(seeds[8], part), 71), part),
        "prompt_length": draw_prompt_length(jax.random.fold_in(jax.random.fold_in(seeds[8], part), 71), part),
        "window_size": draw_window_size(jax.random.fold_in(jax.random.fold_in(seeds[8], part), 71), part),
    }


NEG = -1.0e30


def reference(queries, span_keys, span_values, cache_keys, cache_values, span_start, prompt_length, window_size):
    groups = H // KVH
    scale = HD ** -0.5
    start = span_start[0]
    live = prompt_length[0] - start
    window = window_size[0]
    keys = jnp.concatenate([cache_keys, span_keys], 0).reshape(-1, KVH, HD).astype(jnp.float32)
    values = jnp.concatenate([cache_values, span_values], 0).reshape(-1, KVH, HD).astype(jnp.float32)
    key_pos = jnp.concatenate([start - WINDOW + jnp.arange(WINDOW, dtype=jnp.int32), start + jnp.arange(SPAN, dtype=jnp.int32)]).astype(jnp.int32)
    rows = jnp.arange(SPAN, dtype=jnp.int32)
    query_pos = start + rows
    query_live = rows < live
    diff = query_pos[:, None] - key_pos[None, :]
    valid = (key_pos >= 0)[None, :] & (diff >= 0) & (diff < window) & query_live[:, None]
    grouped = queries.reshape(SPAN, KVH, groups, HD).astype(jnp.float32)

    def one_head(item):
        head_q, head_k, head_v = item
        scores = jnp.einsum('qgd,nd->qgn', head_q, head_k) * scale
        allowed = valid[:, None, :]
        masked = jnp.where(allowed, scores, NEG)
        top = jnp.max(masked, axis=-1, keepdims=True)
        weights = jnp.where(allowed, jnp.exp(scores - top), 0.0)
        total = jnp.sum(weights, axis=-1)
        mixed = jnp.einsum('qgn,nd->qgd', weights.astype(jnp.bfloat16).astype(jnp.float32), head_v)
        safe = jnp.where(query_live[:, None], total, 1.0)
        return jnp.where(query_live[:, None, None], mixed / safe[..., None], 0.0)

    heads = lax.map(one_head, (grouped.transpose(1, 0, 2, 3), keys.transpose(1, 0, 2), values.transpose(1, 0, 2)))
    return heads.transpose(1, 0, 2, 3).reshape(SPAN, H * HD).astype(jnp.bfloat16)
```

```python
import functools

import jax
import jax.numpy as jnp
from jax import lax
from jax.experimental import pallas as pl
from jax.experimental.pallas import tpu as pltpu
from jax.sharding import PartitionSpec as P

HD = 128
NEG = -1e30
FLOOR = -1e29
LOG2E = 1.4426950408889634
MESH = pl.DeviceIdType.MESH


def chunks_of(total, size):
    return [(at, min(size, total - at)) for at in range(0, total, size)]


def grouped(sizes):
    ends = [sum(sizes[: i + 1]) for i in range(len(sizes))]
    return [(end - size, end) for size, end in zip(sizes, ends) if size > 0]


def q_plan(heads):
    return grouped([1, heads // 2 - 1, heads - heads // 2])


def o_plan(heads):
    return grouped([2] * ((heads - 2) // 2) + [1] * (heads - 2 * ((heads - 2) // 2)))


def l_plan(tiles):
    return grouped([tiles - 1, 1])


def kernel(
    n,
    start_hbm,
    length_hbm,
    window_hbm,
    q_hbm,
    sk_hbm,
    sv_hbm,
    ck_hbm,
    cv_hbm,
    out_ref,
    start_ref,
    length_ref,
    window_ref,
    q_own,
    q_got,
    keys,
    values,
    bias,
    scores,
    own_o,
    own_l,
    put_o,
    put_l,
    got_o,
    got_l,
    load_sem,
    own_sem,
    word_sem,
    qs_sem,
    qr_sem,
    os_sem,
    or_sem,
    ls_sem,
    lr_sem,
):
    me = lax.axis_index("seq")
    rows = q_hbm.shape[0]
    cached = ck_hbm.shape[0]
    span = sk_hbm.shape[0]
    total = cached + span
    heads = ck_hbm.shape[1] // HD
    groups = q_hbm.shape[1] // ck_hbm.shape[1]
    wide = groups * rows
    tile = 8 // groups
    factor = HD ** (-0.5) * LOG2E

    def kv_cols(h):
        return pl.ds(pl.multiple_of(h * HD, HD), HD)

    def q_cols(h):
        return pl.ds(pl.multiple_of(h * groups * HD, HD), groups * HD)

    def loads(h):
        return (
            pltpu.make_async_copy(
                ck_hbm.at[:, kv_cols(h)], keys.at[h, pl.ds(0, cached)], load_sem.at[h, 0]
            ),
            pltpu.make_async_copy(
                sk_hbm.at[:, kv_cols(h)], keys.at[h, pl.ds(cached, span)], load_sem.at[h, 1]
            ),
            pltpu.make_async_copy(
                cv_hbm.at[:, kv_cols(h)], values.at[h, pl.ds(0, cached)], load_sem.at[h, 2]
            ),
            pltpu.make_async_copy(
                sv_hbm.at[:, kv_cols(h)], values.at[h, pl.ds(cached, span)], load_sem.at[h, 3]
            ),
        )

    asks = q_plan(heads)
    answers = o_plan(heads)
    tallies = l_plan(heads // tile)

    def ask(d, i):
        across = pl.ds(asks[i][0], asks[i][1] - asks[i][0])
        return pltpu.make_async_remote_copy(
            src_ref=q_own.at[across],
            dst_ref=q_got.at[d - 1, across],
            send_sem=qs_sem.at[d - 1, i],
            recv_sem=qr_sem.at[d - 1, i],
            device_id={"seq": lax.rem(me + d, n)},
            device_id_type=MESH,
        )

    def answer(d, i):
        across = pl.ds(answers[i][0], answers[i][1] - answers[i][0])
        return pltpu.make_async_remote_copy(
            src_ref=put_o.at[d - 1, across],
            dst_ref=got_o.at[d - 1, across],
            send_sem=os_sem.at[d - 1, i],
            recv_sem=or_sem.at[d - 1, i],
            device_id={"seq": lax.rem(me + n - d, n)},
            device_id_type=MESH,
        )

    def answer_l(d, i):
        across = pl.ds(tallies[i][0], tallies[i][1] - tallies[i][0])
        return pltpu.make_async_remote_copy(
            src_ref=put_l.at[d - 1, across],
            dst_ref=got_l.at[d - 1, across],
            send_sem=ls_sem.at[d - 1, i],
            recv_sem=lr_sem.at[d - 1, i],
            device_id={"seq": lax.rem(me + n - d, n)},
            device_id_type=MESH,
        )

    barrier = pltpu.get_barrier_semaphore()
    for d in range(1, n):
        pl.semaphore_signal(
            barrier, inc=1, device_id={"seq": lax.rem(me + d, n)}, device_id_type=MESH
        )
    words = [
        pltpu.make_async_copy(src, dst, word_sem.at[i])
        for i, (src, dst) in enumerate(
            ((start_hbm, start_ref), (length_hbm, length_ref), (window_hbm, window_ref))
        )
    ]

    def own_copy(h):
        return pltpu.make_async_copy(q_hbm.at[:, q_cols(h)], q_own.at[h], own_sem.at[h])

    for h in range(asks[0][1]):
        own_copy(h).start()
    if n > 1:
        pl.semaphore_wait(barrier, n - 1)
    for h in range(asks[0][1]):
        own_copy(h).wait()
    for d in range(1, n):
        ask(d, 0).start()

    @pl.loop(asks[0][1], heads)
    def _(h):
        own_copy(h).start()

    for copy in words:
        copy.start()
    for copy in loads(0):
        copy.start()
    for i in range(1, len(asks)):

        @pl.loop(asks[i][0], asks[i][1])
        def _(h):
            own_copy(h).wait()

        for d in range(1, n):
            ask(d, i).start()

    @pl.loop(1, heads)
    def _(h):
        for copy in loads(h):
            copy.start()

    for copy in words:
        copy.wait()
    start = start_ref[0]
    length = length_ref[0]
    window = window_ref[0]
    for d in range(n):
        source = lax.rem(me + n - d, n)
        q_pos = start + source * rows + lax.broadcasted_iota(jnp.int32, (1, rows), 1)
        high = jnp.where(q_pos < length, q_pos, -1)
        low = jnp.maximum(q_pos - window + 1, 0)
        for at, size in chunks_of(cached, 256):
            k_pos = (
                start
                + (me - n) * cached
                + at
                + lax.broadcasted_iota(jnp.int32, (size, rows), 0)
            )
            seen = (k_pos >= low) & (k_pos <= high)
            bias[d, pl.ds(at, size), :] = jnp.where(seen, 0.0, NEG).astype(jnp.bfloat16)
        k_pos = start + me * span + lax.broadcasted_iota(jnp.int32, (span, rows), 0)
        seen = (k_pos >= low) & (k_pos <= high)
        bias[d, pl.ds(cached, span), :] = jnp.where(seen, 0.0, NEG).astype(jnp.bfloat16)

    parts = chunks_of(cached, 256) + [(cached + at, size) for at, size in chunks_of(span, 256)]

    def unit(d, h, q):
        q_stack = jnp.concatenate(
            [q[:, g * HD : (g + 1) * HD] for g in range(groups)], axis=0
        )
        eye = (
            lax.broadcasted_iota(jnp.int32, (rows, rows), 0)
            == lax.broadcasted_iota(jnp.int32, (rows, rows), 1)
        )
        eye = jnp.where(eye, 1.0, 0.0).astype(jnp.bfloat16)
        q_wide = jnp.concatenate(
            [q_stack, jnp.concatenate([eye] * groups, axis=0)], axis=1
        )
        top = jnp.full((8, wide), FLOOR, jnp.float32)
        for at, size in parts:
            k_wide = jnp.concatenate(
                [keys[h, pl.ds(at, size), :], bias[d, pl.ds(at, size), :]], axis=1
            )
            s = lax.dot_general(
                k_wide, q_wide, (((1,), (1,)), ((), ())), preferred_element_type=jnp.float32
            )
            scores[pl.ds(at, size), :] = s
            top = jnp.maximum(top, jnp.max(s.reshape(size // 8, 8, wide), axis=0))
        top = jnp.max(top, axis=0, keepdims=True)
        sums = jnp.zeros((8, wide), jnp.float32)
        mixed = jnp.zeros((HD, wide), jnp.float32)
        for at, size in parts:
            w = jnp.exp2((scores[pl.ds(at, size), :] - top) * factor)
            sums = sums + jnp.sum(w.reshape(size // 8, 8, wide), axis=0)
            mixed = mixed + lax.dot_general(
                values[h, pl.ds(at, size), :],
                w.astype(jnp.bfloat16),
                (((0,), (0,)), ((), ())),
                preferred_element_type=jnp.float32,
            )
        sums = jnp.sum(sums, axis=0, keepdims=True)
        some = sums > 0.0
        safe = jnp.where(some, sums, 1.0)
        level = jnp.where(some, top * factor + jnp.log2(safe), NEG)
        return mixed / safe, level

    @pl.loop(0, heads)
    def _(h):
        for copy in loads(h):
            copy.wait()
        o, level = unit(0, h, q_own[h])
        own_o[h] = o
        for g in range(groups):
            own_l[h, pl.ds(g, 1), :] = level[:, g * rows : (g + 1) * rows]

        for i, (_, end) in enumerate(answers[:-1]):

            @pl.when(h == end)
            def _(i=i):
                for d in range(1, n):
                    answer(d, i).start()

        for d in range(1, n):
            for i, (first, _) in enumerate(asks):

                @pl.when(h == first)
                def _(d=d, i=i):
                    ask(d, i).wait_recv()

            o, level = unit(d, h, q_got[d - 1, h])
            put_o[d - 1, h] = o.astype(jnp.bfloat16)
            for g in range(groups):
                put_l[d - 1, h // tile, pl.ds(lax.rem(h, tile) * groups + g, 1), :] = level[
                    :, g * rows : (g + 1) * rows
                ]

        for i, (_, end) in enumerate(tallies):

            @pl.when(h == end * tile - 1)
            def _(i=i):
                for d in range(1, n):
                    answer_l(d, i).start()

    for d in range(1, n):
        answer(d, len(answers) - 1).start()

    for i, (first, last) in enumerate(answers):
        for t, (at, _) in enumerate(tallies):
            if first <= at * tile < last:
                for d in range(1, n):
                    answer_l(d, t).wait_recv()
        for d in range(1, n):
            answer(d, i).wait_recv()

        @pl.loop(first, last)
        def _(h):
            for g in range(groups):
                levels = [own_l[h, pl.ds(g, 1), :]] + [
                    got_l[d - 1, h // tile, pl.ds(lax.rem(h, tile) * groups + g, 1), :]
                    for d in range(1, n)
                ]
                best = functools.reduce(jnp.maximum, levels)
                shares = [jnp.exp2(level - best) for level in levels]
                across = pl.ds(g * rows, rows)
                o = own_o[h, :, across] * shares[0]
                for d in range(1, n):
                    o = o + got_o[d - 1, h, :, across].astype(jnp.float32) * shares[d]
                o = o / functools.reduce(jnp.add, shares)
                cols = pl.ds(pl.multiple_of((h * groups + g) * HD, HD), HD)
                out_ref[:, cols] = o.T.astype(jnp.bfloat16)

    for d in range(1, n):
        for i in range(len(asks)):
            ask(d, i).wait_send()
        for i in range(len(answers)):
            answer(d, i).wait_send()
        for i in range(len(tallies)):
            answer_l(d, i).wait_send()


def body(n, queries, span_keys, span_values, cache_keys, cache_values, start, length, window):
    rows = queries.shape[0]
    cached = cache_keys.shape[0]
    span = span_keys.shape[0]
    total = cached + span
    heads = cache_keys.shape[1] // HD
    groups = queries.shape[1] // cache_keys.shape[1]
    wide = groups * rows
    peers = max(n - 1, 1)
    flops = 4 * n * queries.shape[1] * rows * total
    scratch = [
        pltpu.SMEM((1,), jnp.int32),
        pltpu.SMEM((1,), jnp.int32),
        pltpu.SMEM((1,), jnp.int32),
        pltpu.VMEM((heads, rows, groups * HD), jnp.bfloat16),
        pltpu.VMEM((peers, heads, rows, groups * HD), jnp.bfloat16),
        pltpu.VMEM((heads, total, HD), jnp.bfloat16),
        pltpu.VMEM((heads, total, HD), jnp.bfloat16),
        pltpu.VMEM((n, total, rows), jnp.bfloat16),
        pltpu.VMEM((total, wide), jnp.float32),
        pltpu.VMEM((heads, HD, wide), jnp.float32),
        pltpu.VMEM((heads, 8, rows), jnp.float32),
        pltpu.VMEM((peers, heads, HD, wide), jnp.bfloat16),
        pltpu.VMEM((peers, heads * groups // 8, 8, rows), jnp.float32),
        pltpu.VMEM((peers, heads, HD, wide), jnp.bfloat16),
        pltpu.VMEM((peers, heads * groups // 8, 8, rows), jnp.float32),
        pltpu.SemaphoreType.DMA((heads, 4)),
        pltpu.SemaphoreType.DMA((heads,)),
        pltpu.SemaphoreType.DMA((3,)),
        pltpu.SemaphoreType.DMA((peers, len(q_plan(heads)))),
        pltpu.SemaphoreType.DMA((peers, len(q_plan(heads)))),
        pltpu.SemaphoreType.DMA((peers, len(o_plan(heads)))),
        pltpu.SemaphoreType.DMA((peers, len(o_plan(heads)))),
        pltpu.SemaphoreType.DMA((peers, len(l_plan(heads * groups // 8)))),
        pltpu.SemaphoreType.DMA((peers, len(l_plan(heads * groups // 8)))),
    ]
    return pl.pallas_call(
        functools.partial(kernel, n),
        out_shape=pltpu.VMEM(queries.shape, jnp.bfloat16),
        in_specs=[pl.BlockSpec(memory_space=pltpu.HBM)] * 8,
        out_specs=pl.BlockSpec(memory_space=pltpu.VMEM),
        scratch_shapes=scratch,
        compiler_params=pltpu.CompilerParams(
            collective_id=0, has_side_effects=True, vmem_limit_bytes=56 * 1024 * 1024
        ),
        cost_estimate=pl.CostEstimate(
            flops=flops, bytes_accessed=4 * total * HD * heads, transcendentals=flops // (4 * HD)
        ),
        name="windowed",
    )(start, length, window, queries, span_keys, span_values, cache_keys, cache_values)


def solution(mesh):
    both = P(("batch", "seq"), None)
    placed = (both,) * 5 + (P("batch"),) * 3
    return jax.shard_map(
        functools.partial(body, mesh.shape["seq"]),
        mesh=mesh,
        in_specs=placed,
        out_specs=both,
        check_vma=False,
    )
```

```python
import functools

import jax
import jax.numpy as jnp
from jax import lax
from jax.experimental import pallas as pl
from jax.experimental.pallas import tpu as pltpu
from jax.sharding import PartitionSpec as P

HD = 128
NEG = -1e30
FLOOR = -1e29
LOG2E = 1.4426950408889634
MESH = pl.DeviceIdType.MESH


def chunks_of(total, size):
    return [(at, min(size, total - at)) for at in range(0, total, size)]


def grouped(sizes):
    ends = [sum(sizes[: i + 1]) for i in range(len(sizes))]
    return [(end - size, end) for size, end in zip(sizes, ends) if size > 0]


def q_plan(heads):
    return grouped([1, 1, heads // 4, heads - heads // 4 - 2])


def o_plan(heads):
    return grouped([2] * (heads // 4) + [1] * (heads - 2 * (heads // 4)))


def l_plan(tiles):
    return grouped([tiles - 1, 1])


def kernel(
    n,
    words_own,
    q_hbm,
    sk_hbm,
    sv_hbm,
    ck_hbm,
    cv_hbm,
    out_ref,
    words_got,
    q_own,
    q_got,
    keys,
    values,
    bias,
    scores,
    own_o,
    own_l,
    put_o,
    put_l,
    got_o,
    got_l,
    load_sem,
    own_sem,
    ws_sem,
    wr_sem,
    qs_sem,
    qr_sem,
    os_sem,
    or_sem,
    ls_sem,
    lr_sem,
):
    me = lax.axis_index("seq")
    rows = q_hbm.shape[0]
    cached = ck_hbm.shape[0]
    span = sk_hbm.shape[0]
    total = cached + span
    heads = ck_hbm.shape[1] // HD
    groups = q_hbm.shape[1] // ck_hbm.shape[1]
    wide = groups * rows
    tile = 8 // groups
    factor = HD ** (-0.5) * LOG2E

    def kv_cols(h):
        return pl.ds(pl.multiple_of(h * HD, HD), HD)

    def q_cols(h):
        return pl.ds(pl.multiple_of(h * groups * HD, HD), groups * HD)

    def loads(h):
        return (
            pltpu.make_async_copy(
                ck_hbm.at[:, kv_cols(h)], keys.at[h, pl.ds(0, cached)], load_sem.at[h, 0]
            ),
            pltpu.make_async_copy(
                sk_hbm.at[:, kv_cols(h)], keys.at[h, pl.ds(cached, span)], load_sem.at[h, 1]
            ),
            pltpu.make_async_copy(
                cv_hbm.at[:, kv_cols(h)], values.at[h, pl.ds(0, cached)], load_sem.at[h, 2]
            ),
            pltpu.make_async_copy(
                sv_hbm.at[:, kv_cols(h)], values.at[h, pl.ds(cached, span)], load_sem.at[h, 3]
            ),
        )

    asks = q_plan(heads)
    answers = o_plan(heads)
    tallies = l_plan(heads // tile)

    def ask(d, i):
        across = pl.ds(asks[i][0], asks[i][1] - asks[i][0])
        return pltpu.make_async_remote_copy(
            src_ref=q_own.at[across],
            dst_ref=q_got.at[d - 1, across],
            send_sem=qs_sem.at[d - 1, i],
            recv_sem=qr_sem.at[d - 1, i],
            device_id={"seq": lax.rem(me + d, n)},
            device_id_type=MESH,
        )

    def answer(d, i):
        across = pl.ds(answers[i][0], answers[i][1] - answers[i][0])
        return pltpu.make_async_remote_copy(
            src_ref=put_o.at[d - 1, across],
            dst_ref=got_o.at[d - 1, across],
            send_sem=os_sem.at[d - 1, i],
            recv_sem=or_sem.at[d - 1, i],
            device_id={"seq": lax.rem(me + n - d, n)},
            device_id_type=MESH,
        )

    def answer_l(d, i):
        across = pl.ds(tallies[i][0], tallies[i][1] - tallies[i][0])
        return pltpu.make_async_remote_copy(
            src_ref=put_l.at[d - 1, across],
            dst_ref=got_l.at[d - 1, across],
            send_sem=ls_sem.at[d - 1, i],
            recv_sem=lr_sem.at[d - 1, i],
            device_id={"seq": lax.rem(me + n - d, n)},
            device_id_type=MESH,
        )

    barrier = pltpu.get_barrier_semaphore()
    for d in range(1, n):
        pl.semaphore_signal(
            barrier, inc=1, device_id={"seq": lax.rem(me + d, n)}, device_id_type=MESH
        )
    def tell(d):
        return pltpu.make_async_remote_copy(
            src_ref=words_own,
            dst_ref=words_got,
            send_sem=ws_sem.at[d - 1],
            recv_sem=wr_sem.at[0],
            device_id={"seq": lax.rem(me + d, n)},
            device_id_type=MESH,
        )

    def own_copy(h):
        return pltpu.make_async_copy(q_hbm.at[:, q_cols(h)], q_own.at[h], own_sem.at[h])

    for h in range(asks[0][1]):
        own_copy(h).start()
    if n > 1:
        pl.semaphore_wait(barrier, n - 1)
    for h in range(asks[0][1]):
        own_copy(h).wait()

    @pl.when(me == 0)
    def _():
        for d in range(1, n):
            tell(d).start()

    for d in range(1, n):
        ask(d, 0).start()

    @pl.loop(asks[0][1], heads)
    def _(h):
        own_copy(h).start()

    for copy in loads(0):
        copy.start()
    for i in range(1, len(asks)):

        @pl.loop(asks[i][0], asks[i][1])
        def _(h):
            own_copy(h).wait()

        for d in range(1, n):
            ask(d, i).start()

    @pl.loop(1, heads)
    def _(h):
        for copy in loads(h):
            copy.start()

    if n > 1:

        @pl.when(me == 0)
        def _():
            words_got[...] = words_own[...]

        @pl.when(me > 0)
        def _():
            tell(1).wait_recv()

        words = words_got[...]
    else:
        words = words_own[...]
    start, length, window = [
        jnp.concatenate([words[i : i + 1, :]] * (rows // words.shape[1]), axis=1)
        for i in range(3)
    ]
    for d in range(n):
        source = lax.rem(me + n - d, n)
        q_pos = start + source * rows + lax.broadcasted_iota(jnp.int32, (1, rows), 1)
        high = jnp.where(q_pos < length, q_pos, -1)
        low = jnp.maximum(q_pos - window + 1, 0)
        for at, size in chunks_of(cached, 256):
            k_pos = (
                start
                + (me - n) * cached
                + at
                + lax.broadcasted_iota(jnp.int32, (size, rows), 0)
            )
            seen = (k_pos >= low) & (k_pos <= high)
            bias[d, pl.ds(at, size), :] = jnp.where(seen, 0.0, NEG).astype(jnp.bfloat16)
        k_pos = start + me * span + lax.broadcasted_iota(jnp.int32, (span, rows), 0)
        seen = (k_pos >= low) & (k_pos <= high)
        bias[d, pl.ds(cached, span), :] = jnp.where(seen, 0.0, NEG).astype(jnp.bfloat16)

    parts = chunks_of(cached, 256) + [(cached + at, size) for at, size in chunks_of(span, 256)]

    def unit(d, h, q):
        q_stack = jnp.concatenate(
            [q[:, g * HD : (g + 1) * HD] for g in range(groups)], axis=0
        )
        eye = (
            lax.broadcasted_iota(jnp.int32, (rows, rows), 0)
            == lax.broadcasted_iota(jnp.int32, (rows, rows), 1)
        )
        eye = jnp.where(eye, 1.0, 0.0).astype(jnp.bfloat16)
        q_wide = jnp.concatenate(
            [q_stack, jnp.concatenate([eye] * groups, axis=0)], axis=1
        )
        top = jnp.full((8, wide), FLOOR, jnp.float32)
        for at, size in parts:
            k_wide = jnp.concatenate(
                [keys[h, pl.ds(at, size), :], bias[d, pl.ds(at, size), :]], axis=1
            )
            s = lax.dot_general(
                k_wide, q_wide, (((1,), (1,)), ((), ())), preferred_element_type=jnp.float32
            )
            scores[pl.ds(at, size), :] = s
            top = jnp.maximum(top, jnp.max(s.reshape(size // 8, 8, wide), axis=0))
        top = jnp.max(top, axis=0, keepdims=True)
        sums = jnp.zeros((8, wide), jnp.float32)
        mixed = jnp.zeros((HD, wide), jnp.float32)
        for at, size in parts:
            w = jnp.exp2((scores[pl.ds(at, size), :] - top) * factor)
            sums = sums + jnp.sum(w.reshape(size // 8, 8, wide), axis=0)
            mixed = mixed + lax.dot_general(
                values[h, pl.ds(at, size), :],
                w.astype(jnp.bfloat16),
                (((0,), (0,)), ((), ())),
                preferred_element_type=jnp.float32,
            )
        sums = jnp.sum(sums, axis=0, keepdims=True)
        some = sums > 0.0
        safe = jnp.where(some, sums, 1.0)
        level = jnp.where(some, top * factor + jnp.log2(safe), NEG)
        return mixed / safe, level

    @pl.loop(0, heads)
    def _(h):
        for copy in loads(h):
            copy.wait()
        o, level = unit(0, h, q_own[h])
        own_o[h] = o
        for g in range(groups):
            own_l[h, pl.ds(g, 1), :] = level[:, g * rows : (g + 1) * rows]

        for i, (_, end) in enumerate(answers[:-1]):

            @pl.when(h == end)
            def _(i=i):
                for d in range(1, n):
                    answer(d, i).start()

        for d in range(1, n):
            for i, (first, _) in enumerate(asks):

                @pl.when(h == first)
                def _(d=d, i=i):
                    ask(d, i).wait_recv()

            o, level = unit(d, h, q_got[d - 1, h])
            put_o[d - 1, h] = o.astype(jnp.bfloat16)
            for g in range(groups):
                put_l[d - 1, h // tile, pl.ds(lax.rem(h, tile) * groups + g, 1), :] = level[
                    :, g * rows : (g + 1) * rows
                ]

        for i, (_, end) in enumerate(tallies):

            @pl.when(h == end * tile - 1)
            def _(i=i):
                for d in range(1, n):
                    answer_l(d, i).start()

    for d in range(1, n):
        answer(d, len(answers) - 1).start()

    for i, (first, last) in enumerate(answers):
        for t, (at, _) in enumerate(tallies):
            if first <= at * tile < last:
                for d in range(1, n):
                    answer_l(d, t).wait_recv()
        for d in range(1, n):
            answer(d, i).wait_recv()

        @pl.loop(first, last)
        def _(h):
            for g in range(groups):
                levels = [own_l[h, pl.ds(g, 1), :]] + [
                    got_l[d - 1, h // tile, pl.ds(lax.rem(h, tile) * groups + g, 1), :]
                    for d in range(1, n)
                ]
                best = functools.reduce(jnp.maximum, levels)
                shares = [jnp.exp2(level - best) for level in levels]
                across = pl.ds(g * rows, rows)
                o = own_o[h, :, across] * shares[0]
                for d in range(1, n):
                    o = o + got_o[d - 1, h, :, across].astype(jnp.float32) * shares[d]
                o = o / functools.reduce(jnp.add, shares)
                cols = pl.ds(pl.multiple_of((h * groups + g) * HD, HD), HD)
                out_ref[:, cols] = o.T.astype(jnp.bfloat16)

    @pl.when(me == 0)
    def _():
        for d in range(1, n):
            tell(d).wait_send()

    for d in range(1, n):
        for i in range(len(asks)):
            ask(d, i).wait_send()
        for i in range(len(answers)):
            answer(d, i).wait_send()
        for i in range(len(tallies)):
            answer_l(d, i).wait_send()


def tile_of(start, length, window):
    row = lax.broadcasted_iota(jnp.int32, (8, 128), 0)
    return jnp.where(row == 0, start[0], jnp.where(row == 1, length[0], window[0]))


def body(n, queries, span_keys, span_values, cache_keys, cache_values, start, length, window):
    words = lax.cond(
        lax.axis_index("seq") == 0,
        tile_of,
        lambda *_: jnp.zeros((8, 128), jnp.int32),
        start,
        length,
        window,
    )
    rows = queries.shape[0]
    cached = cache_keys.shape[0]
    span = span_keys.shape[0]
    total = cached + span
    heads = cache_keys.shape[1] // HD
    groups = queries.shape[1] // cache_keys.shape[1]
    wide = groups * rows
    peers = max(n - 1, 1)
    flops = 4 * n * queries.shape[1] * rows * total
    scratch = [
        pltpu.VMEM((8, 128), jnp.int32),
        pltpu.VMEM((heads, rows, groups * HD), jnp.bfloat16),
        pltpu.VMEM((peers, heads, rows, groups * HD), jnp.bfloat16),
        pltpu.VMEM((heads, total, HD), jnp.bfloat16),
        pltpu.VMEM((heads, total, HD), jnp.bfloat16),
        pltpu.VMEM((n, total, rows), jnp.bfloat16),
        pltpu.VMEM((total, wide), jnp.float32),
        pltpu.VMEM((heads, HD, wide), jnp.float32),
        pltpu.VMEM((heads, 8, rows), jnp.float32),
        pltpu.VMEM((peers, heads, HD, wide), jnp.bfloat16),
        pltpu.VMEM((peers, heads * groups // 8, 8, rows), jnp.float32),
        pltpu.VMEM((peers, heads, HD, wide), jnp.bfloat16),
        pltpu.VMEM((peers, heads * groups // 8, 8, rows), jnp.float32),
        pltpu.SemaphoreType.DMA((heads, 4)),
        pltpu.SemaphoreType.DMA((heads,)),
        pltpu.SemaphoreType.DMA((peers,)),
        pltpu.SemaphoreType.DMA((1,)),
        pltpu.SemaphoreType.DMA((peers, len(q_plan(heads)))),
        pltpu.SemaphoreType.DMA((peers, len(q_plan(heads)))),
        pltpu.SemaphoreType.DMA((peers, len(o_plan(heads)))),
        pltpu.SemaphoreType.DMA((peers, len(o_plan(heads)))),
        pltpu.SemaphoreType.DMA((peers, len(l_plan(heads * groups // 8)))),
        pltpu.SemaphoreType.DMA((peers, len(l_plan(heads * groups // 8)))),
    ]
    return pl.pallas_call(
        functools.partial(kernel, n),
        out_shape=pltpu.VMEM(queries.shape, jnp.bfloat16),
        in_specs=[pl.BlockSpec(memory_space=pltpu.VMEM)]
        + [pl.BlockSpec(memory_space=pltpu.HBM)] * 5,
        out_specs=pl.BlockSpec(memory_space=pltpu.VMEM),
        scratch_shapes=scratch,
        compiler_params=pltpu.CompilerParams(
            collective_id=0, has_side_effects=True, vmem_limit_bytes=56 * 1024 * 1024
        ),
        cost_estimate=pl.CostEstimate(
            flops=flops, bytes_accessed=4 * total * HD * heads, transcendentals=flops // (4 * HD)
        ),
        name="windowed",
    )(words, queries, span_keys, span_values, cache_keys, cache_values)


def solution(mesh):
    both = P(("batch", "seq"), None)
    placed = (both,) * 5 + (P("batch"),) * 3
    return jax.shard_map(
        functools.partial(body, mesh.shape["seq"]),
        mesh=mesh,
        in_specs=placed,
        out_specs=both,
        check_vma=False,
    )
```

```python
import functools

import jax
import jax.numpy as jnp
from jax import lax
from jax.experimental import pallas as pl
from jax.experimental.pallas import tpu as pltpu
from jax.sharding import PartitionSpec as P

HD = 128
NEG = -1e30
FLOOR = -1e29
LOG2E = 1.4426950408889634
MESH = pl.DeviceIdType.MESH


def chunks_of(total, size):
    return [(at, min(size, total - at)) for at in range(0, total, size)]


def grouped(sizes):
    ends = [sum(sizes[: i + 1]) for i in range(len(sizes))]
    return [(end - size, end) for size, end in zip(sizes, ends) if size > 0]


def q_plan(heads):
    return grouped([1, 1, heads // 4, heads - heads // 4 - 2])


def o_plan(heads):
    return grouped([2] * (heads // 4) + [1] * (heads - 2 * (heads // 4)))


def l_plan(tiles):
    return grouped([tiles - 1, 1])


def kernel(
    n,
    words_own,
    q_hbm,
    sk_hbm,
    sv_hbm,
    ck_hbm,
    cv_hbm,
    out_ref,
    words_got,
    q_own,
    q_got,
    keys,
    values,
    bias,
    scores,
    own_o,
    own_l,
    put_o,
    put_l,
    got_o,
    got_l,
    load_sem,
    own_sem,
    ws_sem,
    wr_sem,
    qs_sem,
    qr_sem,
    os_sem,
    or_sem,
    ls_sem,
    lr_sem,
):
    me = lax.axis_index("seq")
    rows = q_hbm.shape[0]
    cached = ck_hbm.shape[0]
    span = sk_hbm.shape[0]
    total = cached + span
    heads = ck_hbm.shape[1] // HD
    groups = q_hbm.shape[1] // ck_hbm.shape[1]
    wide = groups * rows
    tile = 8 // groups
    factor = HD ** (-0.5) * LOG2E

    def kv_cols(h):
        return pl.ds(pl.multiple_of(h * HD, HD), HD)

    def q_cols(h):
        return pl.ds(pl.multiple_of(h * groups * HD, HD), groups * HD)

    def loads(h):
        return (
            pltpu.make_async_copy(
                ck_hbm.at[:, kv_cols(h)], keys.at[h, pl.ds(0, cached)], load_sem.at[h, 0]
            ),
            pltpu.make_async_copy(
                sk_hbm.at[:, kv_cols(h)], keys.at[h, pl.ds(cached, span)], load_sem.at[h, 1]
            ),
            pltpu.make_async_copy(
                cv_hbm.at[:, kv_cols(h)], values.at[h, pl.ds(0, cached)], load_sem.at[h, 2]
            ),
            pltpu.make_async_copy(
                sv_hbm.at[:, kv_cols(h)], values.at[h, pl.ds(cached, span)], load_sem.at[h, 3]
            ),
        )

    asks = q_plan(heads)
    answers = o_plan(heads)
    tallies = l_plan(heads // tile)

    def ask(d, i):
        across = pl.ds(asks[i][0], asks[i][1] - asks[i][0])
        return pltpu.make_async_remote_copy(
            src_ref=q_own.at[across],
            dst_ref=q_got.at[d - 1, across],
            send_sem=qs_sem.at[d - 1, i],
            recv_sem=qr_sem.at[d - 1, i],
            device_id={"seq": lax.rem(me + d, n)},
            device_id_type=MESH,
        )

    cut = HD * 3 // 8

    def answer_last(d, part):
        across = pl.ds(0, cut) if part == 0 else pl.ds(cut, HD - cut)
        return pltpu.make_async_remote_copy(
            src_ref=put_o.at[d - 1, heads - 1, across],
            dst_ref=got_o.at[d - 1, heads - 1, across],
            send_sem=os_sem.at[d - 1, len(answers) - 1 + part],
            recv_sem=or_sem.at[d - 1, len(answers) - 1 + part],
            device_id={"seq": lax.rem(me + n - d, n)},
            device_id_type=MESH,
        )

    def answer(d, i):
        across = pl.ds(answers[i][0], answers[i][1] - answers[i][0])
        return pltpu.make_async_remote_copy(
            src_ref=put_o.at[d - 1, across],
            dst_ref=got_o.at[d - 1, across],
            send_sem=os_sem.at[d - 1, i],
            recv_sem=or_sem.at[d - 1, i],
            device_id={"seq": lax.rem(me + n - d, n)},
            device_id_type=MESH,
        )

    def answer_l(d, i):
        across = pl.ds(tallies[i][0], tallies[i][1] - tallies[i][0])
        return pltpu.make_async_remote_copy(
            src_ref=put_l.at[d - 1, across],
            dst_ref=got_l.at[d - 1, across],
            send_sem=ls_sem.at[d - 1, i],
            recv_sem=lr_sem.at[d - 1, i],
            device_id={"seq": lax.rem(me + n - d, n)},
            device_id_type=MESH,
        )

    barrier = pltpu.get_barrier_semaphore()
    for d in range(1, n):
        pl.semaphore_signal(
            barrier, inc=1, device_id={"seq": lax.rem(me + d, n)}, device_id_type=MESH
        )
    def tell(d):
        return pltpu.make_async_remote_copy(
            src_ref=words_own,
            dst_ref=words_got,
            send_sem=ws_sem.at[d - 1],
            recv_sem=wr_sem.at[0],
            device_id={"seq": lax.rem(me + d, n)},
            device_id_type=MESH,
        )

    def own_copy(h):
        return pltpu.make_async_copy(q_hbm.at[:, q_cols(h)], q_own.at[h], own_sem.at[h])

    for h in range(asks[0][1]):
        own_copy(h).start()
    if n > 1:
        pl.semaphore_wait(barrier, n - 1)
    for h in range(asks[0][1]):
        own_copy(h).wait()

    @pl.when(me == 0)
    def _():
        for d in range(1, n):
            tell(d).start()

    for d in range(1, n):
        ask(d, 0).start()

    @pl.loop(asks[0][1], heads)
    def _(h):
        own_copy(h).start()

    for copy in loads(0):
        copy.start()
    for i in range(1, len(asks)):

        @pl.loop(asks[i][0], asks[i][1])
        def _(h):
            own_copy(h).wait()

        for d in range(1, n):
            ask(d, i).start()

    @pl.loop(1, heads)
    def _(h):
        for copy in loads(h):
            copy.start()

    if n > 1:

        @pl.when(me == 0)
        def _():
            words_got[...] = words_own[...]

        @pl.when(me > 0)
        def _():
            tell(1).wait_recv()

        words = words_got[...]
    else:
        words = words_own[...]
    start, length, window = [
        jnp.concatenate([words[i : i + 1, :]] * (rows // words.shape[1]), axis=1)
        for i in range(3)
    ]
    for d in range(n):
        source = lax.rem(me + n - d, n)
        q_pos = start + source * rows + lax.broadcasted_iota(jnp.int32, (1, rows), 1)
        high = jnp.where(q_pos < length, q_pos, -1)
        low = jnp.maximum(q_pos - window + 1, 0)
        for at, size in chunks_of(cached, 256):
            k_pos = (
                start
                + (me - n) * cached
                + at
                + lax.broadcasted_iota(jnp.int32, (size, rows), 0)
            )
            seen = (k_pos >= low) & (k_pos <= high)
            bias[d, pl.ds(at, size), :] = jnp.where(seen, 0.0, NEG).astype(jnp.bfloat16)
        k_pos = start + me * span + lax.broadcasted_iota(jnp.int32, (span, rows), 0)
        seen = (k_pos >= low) & (k_pos <= high)
        bias[d, pl.ds(cached, span), :] = jnp.where(seen, 0.0, NEG).astype(jnp.bfloat16)

    parts = chunks_of(cached, 256) + [(cached + at, size) for at, size in chunks_of(span, 256)]

    def unit(d, h, q):
        q_stack = jnp.concatenate(
            [q[:, g * HD : (g + 1) * HD] for g in range(groups)], axis=0
        )
        eye = (
            lax.broadcasted_iota(jnp.int32, (rows, rows), 0)
            == lax.broadcasted_iota(jnp.int32, (rows, rows), 1)
        )
        eye = jnp.where(eye, 1.0, 0.0).astype(jnp.bfloat16)
        q_wide = jnp.concatenate(
            [q_stack, jnp.concatenate([eye] * groups, axis=0)], axis=1
        )
        top = jnp.full((8, wide), FLOOR, jnp.float32)
        for at, size in parts:
            k_wide = jnp.concatenate(
                [keys[h, pl.ds(at, size), :], bias[d, pl.ds(at, size), :]], axis=1
            )
            s = lax.dot_general(
                k_wide, q_wide, (((1,), (1,)), ((), ())), preferred_element_type=jnp.float32
            )
            scores[pl.ds(at, size), :] = s
            top = jnp.maximum(top, jnp.max(s.reshape(size // 8, 8, wide), axis=0))
        top = jnp.max(top, axis=0, keepdims=True)
        sums = jnp.zeros((8, wide), jnp.float32)
        mixed = jnp.zeros((HD, wide), jnp.float32)
        for at, size in parts:
            w = jnp.exp2((scores[pl.ds(at, size), :] - top) * factor)
            sums = sums + jnp.sum(w.reshape(size // 8, 8, wide), axis=0)
            mixed = mixed + lax.dot_general(
                values[h, pl.ds(at, size), :],
                w.astype(jnp.bfloat16),
                (((0,), (0,)), ((), ())),
                preferred_element_type=jnp.float32,
            )
        sums = jnp.sum(sums, axis=0, keepdims=True)
        some = sums > 0.0
        safe = jnp.where(some, sums, 1.0)
        level = jnp.where(some, top * factor + jnp.log2(safe), NEG)
        return mixed / safe, level

    @pl.loop(0, heads)
    def _(h):
        for copy in loads(h):
            copy.wait()
        o, level = unit(0, h, q_own[h])
        own_o[h] = o
        for g in range(groups):
            own_l[h, pl.ds(g, 1), :] = level[:, g * rows : (g + 1) * rows]

        for i, (_, end) in enumerate(answers[:-1]):

            @pl.when(h == end)
            def _(i=i):
                for d in range(1, n):
                    answer(d, i).start()

        for d in range(1, n):
            for i, (first, _) in enumerate(asks):

                @pl.when(h == first)
                def _(d=d, i=i):
                    ask(d, i).wait_recv()

            o, level = unit(d, h, q_got[d - 1, h])
            put_o[d - 1, h] = o.astype(jnp.bfloat16)
            for g in range(groups):
                put_l[d - 1, h // tile, pl.ds(lax.rem(h, tile) * groups + g, 1), :] = level[
                    :, g * rows : (g + 1) * rows
                ]

        for i, (_, end) in enumerate(tallies):

            @pl.when(h == end * tile - 1)
            def _(i=i):
                for d in range(1, n):
                    answer_l(d, i).start()

    core = lax.rem(lax.axis_index("batch"), 2)

    for d in range(1, n):
        answer_last(d, 0).start()

    @pl.when(core == 0)
    def _():
        for d in range(1, n):
            answer_last(d, 1).start()

    for i, (first, last) in enumerate(answers):
        for t, (at, _) in enumerate(tallies):
            if first <= at * tile < last:
                for d in range(1, n):
                    answer_l(d, t).wait_recv()
        for d in range(1, n):
            if i < len(answers) - 1:
                answer(d, i).wait_recv()
            else:
                answer_last(d, 0).wait_recv()
                answer_last(d, 1).wait_recv()
        if i == len(answers) - 2:

            @pl.when(core == 1)
            def _():
                for d in range(1, n):
                    answer_last(d, 1).start()

        @pl.loop(first, last)
        def _(h):
            for g in range(groups):
                levels = [own_l[h, pl.ds(g, 1), :]] + [
                    got_l[d - 1, h // tile, pl.ds(lax.rem(h, tile) * groups + g, 1), :]
                    for d in range(1, n)
                ]
                best = functools.reduce(jnp.maximum, levels)
                shares = [jnp.exp2(level - best) for level in levels]
                across = pl.ds(g * rows, rows)
                o = own_o[h, :, across] * shares[0]
                for d in range(1, n):
                    o = o + got_o[d - 1, h, :, across].astype(jnp.float32) * shares[d]
                o = o / functools.reduce(jnp.add, shares)
                cols = pl.ds(pl.multiple_of((h * groups + g) * HD, HD), HD)
                out_ref[:, cols] = o.T.astype(jnp.bfloat16)

    @pl.when(me == 0)
    def _():
        for d in range(1, n):
            tell(d).wait_send()

    for d in range(1, n):
        for i in range(len(asks)):
            ask(d, i).wait_send()
        for i in range(len(answers) - 1):
            answer(d, i).wait_send()
        for part in range(2):
            answer_last(d, part).wait_send()
        for i in range(len(tallies)):
            answer_l(d, i).wait_send()


def tile_of(start, length, window):
    row = lax.broadcasted_iota(jnp.int32, (8, 128), 0)
    return jnp.where(row == 0, start[0], jnp.where(row == 1, length[0], window[0]))


def body(n, queries, span_keys, span_values, cache_keys, cache_values, start, length, window):
    words = lax.cond(
        lax.axis_index("seq") == 0,
        tile_of,
        lambda *_: jnp.zeros((8, 128), jnp.int32),
        start,
        length,
        window,
    )
    rows = queries.shape[0]
    cached = cache_keys.shape[0]
    span = span_keys.shape[0]
    total = cached + span
    heads = cache_keys.shape[1] // HD
    groups = queries.shape[1] // cache_keys.shape[1]
    wide = groups * rows
    peers = max(n - 1, 1)
    flops = 4 * n * queries.shape[1] * rows * total
    scratch = [
        pltpu.VMEM((8, 128), jnp.int32),
        pltpu.VMEM((heads, rows, groups * HD), jnp.bfloat16),
        pltpu.VMEM((peers, heads, rows, groups * HD), jnp.bfloat16),
        pltpu.VMEM((heads, total, HD), jnp.bfloat16),
        pltpu.VMEM((heads, total, HD), jnp.bfloat16),
        pltpu.VMEM((n, total, rows), jnp.bfloat16),
        pltpu.VMEM((total, wide), jnp.float32),
        pltpu.VMEM((heads, HD, wide), jnp.float32),
        pltpu.VMEM((heads, 8, rows), jnp.float32),
        pltpu.VMEM((peers, heads, HD, wide), jnp.bfloat16),
        pltpu.VMEM((peers, heads * groups // 8, 8, rows), jnp.float32),
        pltpu.VMEM((peers, heads, HD, wide), jnp.bfloat16),
        pltpu.VMEM((peers, heads * groups // 8, 8, rows), jnp.float32),
        pltpu.SemaphoreType.DMA((heads, 4)),
        pltpu.SemaphoreType.DMA((heads,)),
        pltpu.SemaphoreType.DMA((peers,)),
        pltpu.SemaphoreType.DMA((1,)),
        pltpu.SemaphoreType.DMA((peers, len(q_plan(heads)))),
        pltpu.SemaphoreType.DMA((peers, len(q_plan(heads)))),
        pltpu.SemaphoreType.DMA((peers, len(o_plan(heads)) + 1)),
        pltpu.SemaphoreType.DMA((peers, len(o_plan(heads)) + 1)),
        pltpu.SemaphoreType.DMA((peers, len(l_plan(heads * groups // 8)))),
        pltpu.SemaphoreType.DMA((peers, len(l_plan(heads * groups // 8)))),
    ]
    return pl.pallas_call(
        functools.partial(kernel, n),
        out_shape=pltpu.VMEM(queries.shape, jnp.bfloat16),
        in_specs=[pl.BlockSpec(memory_space=pltpu.VMEM)]
        + [pl.BlockSpec(memory_space=pltpu.HBM)] * 5,
        out_specs=pl.BlockSpec(memory_space=pltpu.VMEM),
        scratch_shapes=scratch,
        compiler_params=pltpu.CompilerParams(
            collective_id=0, has_side_effects=True, vmem_limit_bytes=56 * 1024 * 1024
        ),
        cost_estimate=pl.CostEstimate(
            flops=flops, bytes_accessed=4 * total * HD * heads, transcendentals=flops // (4 * HD)
        ),
        name="windowed",
    )(words, queries, span_keys, span_values, cache_keys, cache_values)


def solution(mesh):
    both = P(("batch", "seq"), None)
    placed = (both,) * 5 + (P("batch"),) * 3
    return jax.shard_map(
        functools.partial(body, mesh.shape["seq"]),
        mesh=mesh,
        in_specs=placed,
        out_specs=both,
        check_vma=False,
    )
```

```python
import functools

import jax
import jax.numpy as jnp
from jax import lax
from jax.experimental import pallas as pl
from jax.experimental.pallas import tpu as pltpu
from jax.sharding import PartitionSpec as P

HD = 128
NEG = -1e30
FLOOR = -1e29
LOG2E = 1.4426950408889634
MESH = pl.DeviceIdType.MESH


def chunks_of(total, size):
    return [(at, min(size, total - at)) for at in range(0, total, size)]


def grouped(sizes):
    ends = [sum(sizes[: i + 1]) for i in range(len(sizes))]
    return [(end - size, end) for size, end in zip(sizes, ends) if size > 0]


def q_plan(heads):
    return grouped([1, 1, heads // 4, heads - heads // 4 - 2])


def o_plan(heads):
    return grouped([2] * (heads // 4) + [1] * (heads - 2 * (heads // 4)))


def l_plan(tiles):
    return grouped([tiles - 1, 1])


def kernel(
    n,
    words_own,
    q_hbm,
    sk_hbm,
    sv_hbm,
    ck_hbm,
    cv_hbm,
    out_ref,
    words_got,
    q_own,
    q_got,
    keys,
    values,
    bias,
    scores,
    own_o,
    own_l,
    put_o,
    put_l,
    got_o,
    got_l,
    load_sem,
    own_sem,
    ws_sem,
    wr_sem,
    qs_sem,
    qr_sem,
    os_sem,
    or_sem,
    ls_sem,
    lr_sem,
):
    me = lax.axis_index("seq")
    rows = q_hbm.shape[0]
    cached = ck_hbm.shape[0]
    span = sk_hbm.shape[0]
    total = cached + span
    heads = ck_hbm.shape[1] // HD
    groups = q_hbm.shape[1] // ck_hbm.shape[1]
    wide = groups * rows
    tile = 8 // groups
    factor = HD ** (-0.5) * LOG2E

    def kv_cols(h):
        return pl.ds(pl.multiple_of(h * HD, HD), HD)

    def q_cols(h):
        return pl.ds(pl.multiple_of(h * groups * HD, HD), groups * HD)

    def loads(h):
        return (
            pltpu.make_async_copy(
                ck_hbm.at[:, kv_cols(h)], keys.at[h, pl.ds(0, cached)], load_sem.at[h, 0]
            ),
            pltpu.make_async_copy(
                sk_hbm.at[:, kv_cols(h)], keys.at[h, pl.ds(cached, span)], load_sem.at[h, 1]
            ),
            pltpu.make_async_copy(
                cv_hbm.at[:, kv_cols(h)], values.at[h, pl.ds(0, cached)], load_sem.at[h, 2]
            ),
            pltpu.make_async_copy(
                sv_hbm.at[:, kv_cols(h)], values.at[h, pl.ds(cached, span)], load_sem.at[h, 3]
            ),
        )

    asks = q_plan(heads)
    answers = o_plan(heads)
    tallies = l_plan(heads // tile)

    def ask(d, i):
        across = pl.ds(asks[i][0], asks[i][1] - asks[i][0])
        return pltpu.make_async_remote_copy(
            src_ref=q_own.at[across],
            dst_ref=q_got.at[d - 1, across],
            send_sem=qs_sem.at[d - 1, i],
            recv_sem=qr_sem.at[d - 1, i],
            device_id={"seq": lax.rem(me + d, n)},
            device_id_type=MESH,
        )

    cut = HD // 4

    def answer_last(d, part):
        across = pl.ds(0, cut) if part == 0 else pl.ds(cut, HD - cut)
        return pltpu.make_async_remote_copy(
            src_ref=put_o.at[d - 1, heads - 1, across],
            dst_ref=got_o.at[d - 1, heads - 1, across],
            send_sem=os_sem.at[d - 1, len(answers) - 1 + part],
            recv_sem=or_sem.at[d - 1, len(answers) - 1 + part],
            device_id={"seq": lax.rem(me + n - d, n)},
            device_id_type=MESH,
        )

    def answer(d, i):
        across = pl.ds(answers[i][0], answers[i][1] - answers[i][0])
        return pltpu.make_async_remote_copy(
            src_ref=put_o.at[d - 1, across],
            dst_ref=got_o.at[d - 1, across],
            send_sem=os_sem.at[d - 1, i],
            recv_sem=or_sem.at[d - 1, i],
            device_id={"seq": lax.rem(me + n - d, n)},
            device_id_type=MESH,
        )

    def answer_l(d, i):
        across = pl.ds(tallies[i][0], tallies[i][1] - tallies[i][0])
        return pltpu.make_async_remote_copy(
            src_ref=put_l.at[d - 1, across],
            dst_ref=got_l.at[d - 1, across],
            send_sem=ls_sem.at[d - 1, i],
            recv_sem=lr_sem.at[d - 1, i],
            device_id={"seq": lax.rem(me + n - d, n)},
            device_id_type=MESH,
        )

    barrier = pltpu.get_barrier_semaphore()
    for d in range(1, n):
        pl.semaphore_signal(
            barrier, inc=1, device_id={"seq": lax.rem(me + d, n)}, device_id_type=MESH
        )
    def tell(d):
        return pltpu.make_async_remote_copy(
            src_ref=words_own,
            dst_ref=words_got,
            send_sem=ws_sem.at[d - 1],
            recv_sem=wr_sem.at[0],
            device_id={"seq": lax.rem(me + d, n)},
            device_id_type=MESH,
        )

    def own_copy(h):
        return pltpu.make_async_copy(q_hbm.at[:, q_cols(h)], q_own.at[h], own_sem.at[h])

    for h in range(asks[0][1]):
        own_copy(h).start()
    if n > 1:
        pl.semaphore_wait(barrier, n - 1)
    for h in range(asks[0][1]):
        own_copy(h).wait()

    @pl.when(me == 0)
    def _():
        for d in range(1, n):
            tell(d).start()

    for d in range(1, n):
        ask(d, 0).start()

    @pl.loop(asks[0][1], heads)
    def _(h):
        own_copy(h).start()

    for copy in loads(0):
        copy.start()
    for i in range(1, len(asks)):

        @pl.loop(asks[i][0], asks[i][1])
        def _(h):
            own_copy(h).wait()

        for d in range(1, n):
            ask(d, i).start()

    @pl.loop(1, heads)
    def _(h):
        for copy in loads(h):
            copy.start()

    if n > 1:

        @pl.when(me == 0)
        def _():
            words_got[...] = words_own[...]

        @pl.when(me > 0)
        def _():
            tell(1).wait_recv()

        words = words_got[...]
    else:
        words = words_own[...]
    start, length, window = [
        jnp.concatenate([words[i : i + 1, :]] * (rows // words.shape[1]), axis=1)
        for i in range(3)
    ]
    for d in range(n):
        source = lax.rem(me + n - d, n)
        q_pos = start + source * rows + lax.broadcasted_iota(jnp.int32, (1, rows), 1)
        high = jnp.where(q_pos < length, q_pos, -1)
        low = jnp.maximum(q_pos - window + 1, 0)
        for at, size in chunks_of(cached, 256):
            k_pos = (
                start
                + (me - n) * cached
                + at
                + lax.broadcasted_iota(jnp.int32, (size, rows), 0)
            )
            seen = (k_pos >= low) & (k_pos <= high)
            bias[d, pl.ds(at, size), :] = jnp.where(seen, 0.0, NEG).astype(jnp.bfloat16)
        k_pos = start + me * span + lax.broadcasted_iota(jnp.int32, (span, rows), 0)
        seen = (k_pos >= low) & (k_pos <= high)
        bias[d, pl.ds(cached, span), :] = jnp.where(seen, 0.0, NEG).astype(jnp.bfloat16)

    parts = chunks_of(cached, 256) + [(cached + at, size) for at, size in chunks_of(span, 256)]

    def unit(d, h, q):
        q_stack = jnp.concatenate(
            [q[:, g * HD : (g + 1) * HD] for g in range(groups)], axis=0
        )
        eye = (
            lax.broadcasted_iota(jnp.int32, (rows, rows), 0)
            == lax.broadcasted_iota(jnp.int32, (rows, rows), 1)
        )
        eye = jnp.where(eye, 1.0, 0.0).astype(jnp.bfloat16)
        q_wide = jnp.concatenate(
            [q_stack, jnp.concatenate([eye] * groups, axis=0)], axis=1
        )
        top = jnp.full((8, wide), FLOOR, jnp.float32)
        for at, size in parts:
            k_wide = jnp.concatenate(
                [keys[h, pl.ds(at, size), :], bias[d, pl.ds(at, size), :]], axis=1
            )
            s = lax.dot_general(
                k_wide, q_wide, (((1,), (1,)), ((), ())), preferred_element_type=jnp.float32
            )
            scores[pl.ds(at, size), :] = s
            top = jnp.maximum(top, jnp.max(s.reshape(size // 8, 8, wide), axis=0))
        top = jnp.max(top, axis=0, keepdims=True)
        sums = jnp.zeros((8, wide), jnp.float32)
        mixed = jnp.zeros((HD, wide), jnp.float32)
        for at, size in parts:
            w = jnp.exp2((scores[pl.ds(at, size), :] - top) * factor)
            sums = sums + jnp.sum(w.reshape(size // 8, 8, wide), axis=0)
            mixed = mixed + lax.dot_general(
                values[h, pl.ds(at, size), :],
                w.astype(jnp.bfloat16),
                (((0,), (0,)), ((), ())),
                preferred_element_type=jnp.float32,
            )
        sums = jnp.sum(sums, axis=0, keepdims=True)
        some = sums > 0.0
        safe = jnp.where(some, sums, 1.0)
        level = jnp.where(some, top * factor + jnp.log2(safe), NEG)
        return mixed / safe, level

    @pl.loop(0, heads)
    def _(h):
        for copy in loads(h):
            copy.wait()
        o, level = unit(0, h, q_own[h])
        own_o[h] = o
        for g in range(groups):
            own_l[h, pl.ds(g, 1), :] = level[:, g * rows : (g + 1) * rows]

        for i, (_, end) in enumerate(answers[:-1]):

            @pl.when(h == end)
            def _(i=i):
                for d in range(1, n):
                    answer(d, i).start()

        for d in range(1, n):
            for i, (first, _) in enumerate(asks):

                @pl.when(h == first)
                def _(d=d, i=i):
                    ask(d, i).wait_recv()

            o, level = unit(d, h, q_got[d - 1, h])
            put_o[d - 1, h] = o.astype(jnp.bfloat16)
            for g in range(groups):
                put_l[d - 1, h // tile, pl.ds(lax.rem(h, tile) * groups + g, 1), :] = level[
                    :, g * rows : (g + 1) * rows
                ]

        for i, (_, end) in enumerate(tallies):

            @pl.when(h == end * tile - 1)
            def _(i=i):
                for d in range(1, n):
                    answer_l(d, i).start()

    core = lax.rem(lax.axis_index("batch"), 2)

    for d in range(1, n):
        answer_last(d, 0).start()

    @pl.when(core == 0)
    def _():
        for d in range(1, n):
            answer_last(d, 1).start()

    for i, (first, last) in enumerate(answers):
        for t, (at, _) in enumerate(tallies):
            if first <= at * tile < last:
                for d in range(1, n):
                    answer_l(d, t).wait_recv()
        for d in range(1, n):
            if i < len(answers) - 1:
                answer(d, i).wait_recv()
            else:
                answer_last(d, 0).wait_recv()
                answer_last(d, 1).wait_recv()
        if i == len(answers) - 2:

            @pl.when(core == 1)
            def _():
                for d in range(1, n):
                    answer_last(d, 1).start()

        @pl.loop(first, last)
        def _(h):
            for g in range(groups):
                levels = [own_l[h, pl.ds(g, 1), :]] + [
                    got_l[d - 1, h // tile, pl.ds(lax.rem(h, tile) * groups + g, 1), :]
                    for d in range(1, n)
                ]
                best = functools.reduce(jnp.maximum, levels)
                shares = [jnp.exp2(level - best) for level in levels]
                across = pl.ds(g * rows, rows)
                o = own_o[h, :, across] * shares[0]
                for d in range(1, n):
                    o = o + got_o[d - 1, h, :, across].astype(jnp.float32) * shares[d]
                o = o / functools.reduce(jnp.add, shares)
                cols = pl.ds(pl.multiple_of((h * groups + g) * HD, HD), HD)
                out_ref[:, cols] = o.T.astype(jnp.bfloat16)

    @pl.when(me == 0)
    def _():
        for d in range(1, n):
            tell(d).wait_send()

    for d in range(1, n):
        for i in range(len(asks)):
            ask(d, i).wait_send()
        for i in range(len(answers) - 1):
            answer(d, i).wait_send()
        for part in range(2):
            answer_last(d, part).wait_send()
        for i in range(len(tallies)):
            answer_l(d, i).wait_send()


def tile_of(start, length, window):
    row = lax.broadcasted_iota(jnp.int32, (8, 128), 0)
    return jnp.where(row == 0, start[0], jnp.where(row == 1, length[0], window[0]))


def body(n, queries, span_keys, span_values, cache_keys, cache_values, start, length, window):
    words = lax.cond(
        lax.axis_index("seq") == 0,
        tile_of,
        lambda *_: jnp.zeros((8, 128), jnp.int32),
        start,
        length,
        window,
    )
    rows = queries.shape[0]
    cached = cache_keys.shape[0]
    span = span_keys.shape[0]
    total = cached + span
    heads = cache_keys.shape[1] // HD
    groups = queries.shape[1] // cache_keys.shape[1]
    wide = groups * rows
    peers = max(n - 1, 1)
    flops = 4 * n * queries.shape[1] * rows * total
    scratch = [
        pltpu.VMEM((8, 128), jnp.int32),
        pltpu.VMEM((heads, rows, groups * HD), jnp.bfloat16),
        pltpu.VMEM((peers, heads, rows, groups * HD), jnp.bfloat16),
        pltpu.VMEM((heads, total, HD), jnp.bfloat16),
        pltpu.VMEM((heads, total, HD), jnp.bfloat16),
        pltpu.VMEM((n, total, rows), jnp.bfloat16),
        pltpu.VMEM((total, wide), jnp.float32),
        pltpu.VMEM((heads, HD, wide), jnp.float32),
        pltpu.VMEM((heads, 8, rows), jnp.float32),
        pltpu.VMEM((peers, heads, HD, wide), jnp.bfloat16),
        pltpu.VMEM((peers, heads * groups // 8, 8, rows), jnp.float32),
        pltpu.VMEM((peers, heads, HD, wide), jnp.bfloat16),
        pltpu.VMEM((peers, heads * groups // 8, 8, rows), jnp.float32),
        pltpu.SemaphoreType.DMA((heads, 4)),
        pltpu.SemaphoreType.DMA((heads,)),
        pltpu.SemaphoreType.DMA((peers,)),
        pltpu.SemaphoreType.DMA((1,)),
        pltpu.SemaphoreType.DMA((peers, len(q_plan(heads)))),
        pltpu.SemaphoreType.DMA((peers, len(q_plan(heads)))),
        pltpu.SemaphoreType.DMA((peers, len(o_plan(heads)) + 1)),
        pltpu.SemaphoreType.DMA((peers, len(o_plan(heads)) + 1)),
        pltpu.SemaphoreType.DMA((peers, len(l_plan(heads * groups // 8)))),
        pltpu.SemaphoreType.DMA((peers, len(l_plan(heads * groups // 8)))),
    ]
    return pl.pallas_call(
        functools.partial(kernel, n),
        out_shape=pltpu.VMEM(queries.shape, jnp.bfloat16),
        in_specs=[pl.BlockSpec(memory_space=pltpu.VMEM)]
        + [pl.BlockSpec(memory_space=pltpu.HBM)] * 5,
        out_specs=pl.BlockSpec(memory_space=pltpu.VMEM),
        scratch_shapes=scratch,
        compiler_params=pltpu.CompilerParams(
            collective_id=0, has_side_effects=True, vmem_limit_bytes=56 * 1024 * 1024
        ),
        cost_estimate=pl.CostEstimate(
            flops=flops, bytes_accessed=4 * total * HD * heads, transcendentals=flops // (4 * HD)
        ),
        name="windowed",
    )(words, queries, span_keys, span_values, cache_keys, cache_values)


def solution(mesh):
    both = P(("batch", "seq"), None)
    placed = (both,) * 5 + (P("batch"),) * 3
    return jax.shard_map(
        functools.partial(body, mesh.shape["seq"]),
        mesh=mesh,
        in_specs=placed,
        out_specs=both,
        check_vma=False,
    )
```
